256 devices in a mesh: scan: 2 (over y), slab: 128 (over z, x, core).
Axes of the slice: x: 4, y: 2, z: 16, core: 2. Of those that a mesh axis runs over, the one named last changes fastest.
The devices are a block of a 4x16x16 slice.
Arguments:
- image: float32 [2, 128, 256, 128], P(None, 'slab', 'scan'), parts along dimension 2, may hold values from -6 to 6
- sensitivity: bfloat16 [12, 2, 128, 128, 128], P('scan', None, 'slab'), parts along dimension 0, may hold values from -1.5 to 1.5
- kernel: float32 [256, 256, 256], P(None, 'slab'), may hold values from 0.1 to 4
Outputs:
- normal_image: float32 [2, 128, 256, 128], P(None, 'slab', 'scan'), parts along dimension 2
The draws below stay inside these ranges and needn't reach their ends.
There are 2 independent parts, one for each index of `scan`. The reference program is written for one: setup_inputs(seed, part) draws one part's arguments, and reference() takes and returns one part's arrays. A program takes and returns all parts, laid end to end along the dimension named above; an argument that names none is the same for every part. Nothing has to cross between parts.
All inputs are finite; a program needn't handle non-finite values.
Results may differ from the reference program's by a relative error of at most 0.0024.
Values may be sent and summed in bfloat16 or wider, within the bound.
No kernel may reach another device: no remote copies, remote signals or barrier semaphores. Data moves between devices by JAX's collectives and lax.ppermute only.
A program may use at most 64 MiB of HBM per device.

```python
import math
import jax
import jax.numpy as jnp
from jax import lax

NX = 128
NY = 128
NZ = 128
COILS = 6
GX = 256
GY = 256
GZ = 256


def block_levels(key, shape, pieces, smallest, top_value):
    level, own = 1.0, jax.random.fold_in(key, 6)
    for dim, shards_of in pieces:
        draws = jnp.exp(jax.random.uniform(jax.random.fold_in(own, dim), (shards_of,), jnp.float32, smallest / len(pieces), top_value / len(pieces)))
        level = level * jnp.repeat(draws, shape[dim] // shards_of).reshape([-1 if axis == dim else 1 for axis in range(len(shape))])
    return level


def gaussian(own_key, extent, deviation, bound, cuts=(), held_as=jnp.bfloat16):
    values = deviation * jax.random.normal(own_key, extent, jnp.float32)
    if cuts:
        values = values * block_levels(own_key, extent, cuts, -0.22, 0.18)
    return jnp.clip(values, -bound, bound).astype(held_as)


def setup_inputs(seed: int = 0, part: int = 0) -> dict:
    streams_of = jax.random.split(jax.random.key(seed), 4)
    part_splits = jax.random.split(jax.random.fold_in(streams_of[3], part), 4)
    return {
        "image": gaussian(part_splits[0], (2, NX, NY, NZ), 1.0, 6.0, ((1, 128),), jnp.float32),
        "sensitivity": gaussian(part_splits[1], (COILS, 2, NX, NY, NZ), 0.25, 1.5, ((2, 128),)),
        "kernel": jnp.clip(jnp.exp(math.log(4.0) - 3.6888794 * jax.random.uniform(streams_of[2], (GX, GY, GZ), jnp.float32) ** block_levels(streams_of[2], (GX, GY, GZ), ((1, 128),), -0.2, 0.2)), 0.1, 4.0),
    }


smooth_weight = 0.1

def fourier_table(count_out, count_in, length, sign_value):
    row_index = lax.broadcasted_iota(jnp.int32, (count_out, count_in), 0)
    column_index = lax.broadcasted_iota(jnp.int32, (count_out, count_in), 1)
    phases = row_index * column_index % length
    angles = phases.astype(jnp.float32) * (2.0 * math.pi / length)
    factor = 1.0 / math.sqrt(length)
    real_part = jnp.cos(angles) * factor
    imaginary = sign_value * jnp.sin(angles) * factor
    stacked = jnp.stack([jnp.stack([real_part, -imaginary]), jnp.stack([imaginary, real_part])])
    return stacked.astype(jnp.bfloat16)

def transform(matrix, values, pattern):
    return jnp.einsum(pattern, matrix.astype(jnp.float32), values.astype(jnp.float32))

def reference(image, sensitivity, kernel):
    forward_first = fourier_table(GX, NX, GX, -1.0)
    forward_second = fourier_table(GY, NY, GY, -1.0)
    forward_third = fourier_table(GZ, NZ, GZ, -1.0)
    inverse_first = fourier_table(NX, GX, GX, 1.0)
    inverse_second = fourier_table(NY, GY, GY, 1.0)
    inverse_third = fourier_table(NZ, GZ, GZ, 1.0)

    def one_coil(accumulated, coil_maps):
        coil_real = coil_maps[0].astype(jnp.float32)
        coil_imaginary = coil_maps[1].astype(jnp.float32)
        coil_image = jnp.stack([coil_real * image[0] - coil_imaginary * image[1], coil_real * image[1] + coil_imaginary * image[0]]).astype(jnp.bfloat16)
        along_second = transform(forward_second, coil_image, 'pqkj,qajb->pakb').astype(jnp.bfloat16)
        along_third = transform(forward_third, along_second, 'pqkj,qabj->pabk').astype(jnp.bfloat16)
        spectrum = transform(forward_first, along_third, 'pqkj,qjab->pkab')
        filtered = (spectrum * kernel).astype(jnp.bfloat16)
        back_first = transform(inverse_first, filtered, 'pqkj,qjab->pkab').astype(jnp.bfloat16)
        back_third = transform(inverse_third, back_first, 'pqkj,qabj->pabk').astype(jnp.bfloat16)
        coil_result = transform(inverse_second, back_third, 'pqkj,qajb->pakb')
        accumulated = accumulated + jnp.stack([coil_real * coil_result[0] + coil_imaginary * coil_result[1], coil_real * coil_result[1] - coil_imaginary * coil_result[0]])
        return (accumulated, None)
    accumulated = lax.scan(one_coil, jnp.zeros(image.shape, jnp.float32), sensitivity)[0]
    padded = jnp.pad(image, ((0, 0), (1, 1), (1, 1), (1, 1)))
    beside = padded[:, 2:, 1:-1, 1:-1] + padded[:, :-2, 1:-1, 1:-1]
    beside = beside + padded[:, 1:-1, 2:, 1:-1] + padded[:, 1:-1, :-2, 1:-1]
    beside = beside + padded[:, 1:-1, 1:-1, 2:] + padded[:, 1:-1, 1:-1, :-2]
    penalty = 6.0 * image - beside
    return accumulated + smooth_weight * penalty
```

```python
import functools
import math

import jax
import jax.numpy as jnp
import ml_dtypes
import numpy as np
from jax import lax
from jax.experimental import pallas as pl
from jax.experimental.pallas import tpu as pltpu
from jax.sharding import Mesh
from jax.sharding import PartitionSpec as P

smooth_weight = 0.1
LAG_NS = 20000
VMEM, SMEM = pltpu.VMEM, pltpu.SMEM


def factor(count_out, count_in, length, sign_value):
    phases = np.outer(np.arange(count_out), np.arange(count_in)) % length
    angles = phases * (2.0 * math.pi / length)
    scale = 1.0 / math.sqrt(length)
    return np.cos(angles) * scale, sign_value * np.sin(angles) * scale


def held(table):
    return table.astype(np.float32).astype(ml_dtypes.bfloat16)


def stacked(real, imaginary):
    return np.block([[real, -imaginary], [imaginary, real]])


def second_tables(size, length, pair):
    real, imaginary = factor(length, size, length, -1.0)
    forward = np.stack(
        [np.concatenate([real, -imaginary], 1), np.concatenate([imaginary, real], 1)], 1
    )
    back_real, back_imaginary = factor(size, length, length, 1.0)
    inverse = np.stack(
        [
            np.concatenate([back_real, back_imaginary], 0),
            np.concatenate([-back_imaginary, back_real], 0),
        ],
        2,
    )
    base = np.arange(length).reshape(-1, 2, pair)
    orders = [base[:, ::step].reshape(-1) for step in (1, -1)]
    return (
        held(np.stack([forward[order].reshape(2 * length, 2 * size) for order in orders])),
        held(np.stack([inverse[:, order].reshape(2 * size, 2 * length) for order in orders])),
    )


def product(a, b):
    return jnp.dot(a, b, preferred_element_type=jnp.float32)


def coil_image_kernel(core_ref, image_ref, sensitivity_ref, own_ref, other_ref):
    core = core_ref[0]
    coils = own_ref.shape[0]
    image_real, image_imaginary = image_ref[0, 0], image_ref[1, 0]
    rows = image_real.shape[0]
    for ref, first in ((other_ref, (1 - core) * coils), (own_ref, core * coils)):
        for coil in range(coils):
            real = sensitivity_ref[first + coil, 0, 0].astype(jnp.float32)
            imaginary = sensitivity_ref[first + coil, 1, 0].astype(jnp.float32)
            ref[coil, :rows] = (real * image_real - imaginary * image_imaginary).astype(ref.dtype)
            ref[coil, rows:] = (real * image_imaginary + imaginary * image_real).astype(ref.dtype)


def second_kernel(core_ref, table_ref, own_ref, other_ref, out_ref):
    core = core_ref[0]
    groups, _, coils, rows, width = out_ref.shape
    table = table_ref[core]
    for ref, slot in ((own_ref, core), (other_ref, 1 - core)):
        for coil in range(coils):
            out_ref[:, slot, coil] = (
                product(table, ref[coil]).reshape(groups, rows, width).astype(out_ref.dtype)
            )

    @pl.when(core == 1)
    def _():
        pl.delay(LAG_NS)


def middle_kernel(
    in_ref, own_ref, other_ref, third_ref, first_ref, back_first_ref, back_third_ref,
    out_ref, lines, spread, filtered, back,
):
    count, coils, rows, width = in_ref.shape
    grid = own_ref.shape[0]
    frequencies = rows // 2

    @pl.loop(0, coils)
    def _(coil):
        lines[...] = in_ref[:, coil].astype(jnp.float32).reshape(count * rows, width)
        for j in range(frequencies):
            both = jnp.concatenate(
                [lines[pl.ds(2 * j + part, count, stride=rows), :] for part in range(2)], axis=1
            ).astype(jnp.bfloat16)
            third = product(both, third_ref[...]).astype(jnp.bfloat16)
            spread[:count] = third[:, :grid]
            spread[count:] = third[:, grid:]
            points_ref = (own_ref, other_ref)[j // (frequencies // 2)]
            at = j % (frequencies // 2) * grid
            points = points_ref[:, at : at + grid]
            for part in range(2):
                spectrum = product(first_ref[part * grid : (part + 1) * grid], spread[...])
                filtered[part * grid : (part + 1) * grid] = (spectrum * points).astype(jnp.bfloat16)
            first = product(back_first_ref[...], filtered[...]).astype(jnp.bfloat16)
            back[:, :grid] = first[:count]
            back[:, grid:] = first[count:]
            result = product(back[...], back_third_ref[...])
            for part in range(2):
                lines[pl.ds(2 * j + part, count, stride=rows), :] = result[
                    :, part * width : (part + 1) * width
                ]
        out_ref[:, coil] = lines[...].reshape(count, rows, width).astype(out_ref.dtype)


def last_kernel(core_ref, in_ref, table_ref, sensitivity_ref, out_ref, *, own):
    core = core_ref[0]
    groups, _, coils, rows, width = in_ref.shape
    table = table_ref[core]
    slot = core if own else 1 - core
    first = core * coils if own else 0
    size = table.shape[0] // 2
    real_sum = imaginary_sum = 0.0
    for coil in range(coils):
        values = product(table, in_ref[:, slot, coil].reshape(groups * rows, width))
        real = sensitivity_ref[first + coil, 0, 0].astype(jnp.float32)
        imaginary = sensitivity_ref[first + coil, 1, 0].astype(jnp.float32)
        real_sum += real * values[:size] + imaginary * values[size:]
        imaginary_sum += real * values[size:] - imaginary * values[:size]
    out_ref[0, 0] = real_sum
    out_ref[1, 0] = imaginary_sum


def call(kernel, name, out, spaces, operands, scratch=(), flops=0, mib=8):
    return pl.pallas_call(
        kernel,
        name=name,
        out_shape=out,
        in_specs=[pl.BlockSpec(memory_space=space) for space in spaces],
        out_specs=jax.tree.map(lambda _: pl.BlockSpec(memory_space=VMEM), out),
        scratch_shapes=scratch,
        compiler_params=pltpu.CompilerParams(vmem_limit_bytes=mib * 2**20),
        cost_estimate=pl.CostEstimate(flops=flops, bytes_accessed=2**20, transcendentals=0),
    )(*operands)


def local(image, sensitivity, kernel, *, groups, size):
    bf16, f32 = jnp.bfloat16, jnp.float32
    coils, width = sensitivity.shape[0] // 2, image.shape[3]
    grid, pair = kernel.shape[0], kernel.shape[1]
    rows = 4 * pair
    core = lax.axis_index("core")
    where = core.astype(jnp.int32).reshape(1)
    swap = [(0, 1), (1, 0)]
    shape = jax.ShapeDtypeStruct

    forward_second, inverse_second = second_tables(size, grid, pair)
    forward = factor(grid, size, grid, -1.0)
    inverse = factor(size, grid, grid, 1.0)
    first_table, back_first_table = held(stacked(*forward)), held(stacked(*inverse))
    third_table, back_third_table = held(stacked(*forward).T), held(stacked(*inverse).T)

    own_coils, other_coils = call(
        coil_image_kernel, "coil_images",
        (shape((coils, 2 * size, width), bf16),) * 2,
        (SMEM, VMEM, VMEM), (where, image, sensitivity), flops=2**20,
    )
    partner_coils = lax.ppermute(other_coils, "core", swap)
    sent = lax.dynamic_slice_in_dim(sensitivity, (1 - core) * coils, coils, 0)
    partner_sensitivity = lax.ppermute(sent, "core", swap)
    partner_image = lax.ppermute(image, "core", swap)
    own_coils, partner_coils, own_points, partner_points = lax.optimization_barrier(
        (own_coils, partner_coils, kernel, lax.ppermute(kernel, "core", swap))
    )
    own_points = own_points.reshape(grid, pair * grid)
    partner_points = partner_points.reshape(grid, pair * grid)

    payload = call(
        second_kernel, "along_second",
        shape((groups, 2, coils, rows, width), bf16),
        (SMEM, VMEM, VMEM, VMEM), (where, forward_second, own_coils, partner_coils), flops=2**28,
    )
    received = lax.all_to_all(payload, "chip", split_axis=0, concat_axis=0, tiled=True)
    returned = call(
        middle_kernel, "middle",
        shape((size, coils, rows, width), bf16),
        (VMEM,) * 7,
        (received.reshape(size, coils, rows, width), own_points, partner_points,
         third_table, first_table, back_first_table, back_third_table),
        (pltpu.VMEM((size * rows, width), f32), pltpu.VMEM((2 * size, grid), bf16),
         pltpu.VMEM((2 * grid, grid), bf16), pltpu.VMEM((size, 2 * grid), bf16)),
        flops=2**31, mib=16,
    )
    returned = lax.all_to_all(
        returned.reshape(groups, 2, coils, rows, width), "chip", split_axis=0, concat_axis=0, tiled=True
    )
    sums = [
        call(
            functools.partial(last_kernel, own=own), "along_second_back",
            shape(image.shape, f32), (SMEM, VMEM, VMEM, VMEM),
            (where, returned, inverse_second, weights), flops=2**28,
        )
        for own, weights in ((False, partner_sensitivity), (True, sensitivity))
    ]
    partner_sum = lax.ppermute(sums[0], "core", swap)

    ends = 2 * groups - 1
    outer = lax.ppermute(
        image,
        ("chip", "core"),
        [(i, i + 1) for i in range(1, ends, 2)] + [(i, i - 1) for i in range(2, ends + 1, 2)],
    )
    beside = partner_image + outer
    padded = jnp.pad(image, ((0, 0), (0, 0), (1, 1), (1, 1)))
    beside = beside + padded[:, :, 2:, 1:-1] + padded[:, :, :-2, 1:-1]
    beside = beside + padded[:, :, 1:-1, 2:] + padded[:, :, 1:-1, :-2]
    return sums[1] + partner_sum + smooth_weight * (6.0 * image - beside)


def solution(mesh):
    scans, slabs = mesh.devices.shape
    chips = Mesh(mesh.devices.reshape(scans, slabs // 2, 2), (mesh.axis_names[0], "chip", "core"))
    slab = ("chip", "core")
    return jax.shard_map(
        functools.partial(local, groups=slabs // 2, size=slabs),
        mesh=chips,
        in_specs=(
            P(None, slab, mesh.axis_names[0], None),
            P(mesh.axis_names[0], None, slab, None, None),
            P(None, slab, None),
        ),
        out_specs=P(None, slab, mesh.axis_names[0], None),
        check_vma=False,
    )
```

```python
import functools
import math

import jax
import jax.numpy as jnp
import ml_dtypes
import numpy as np
from jax import lax
from jax.experimental import pallas as pl
from jax.experimental.pallas import tpu as pltpu
from jax.sharding import Mesh
from jax.sharding import PartitionSpec as P

smooth_weight = 0.1
LAG_NS = 18000
VMEM, SMEM, HBM = pltpu.VMEM, pltpu.SMEM, pltpu.HBM


def factor(count_out, count_in, length, sign_value):
    phases = np.outer(np.arange(count_out), np.arange(count_in)) % length
    angles = phases * (2.0 * math.pi / length)
    scale = 1.0 / math.sqrt(length)
    return np.cos(angles) * scale, sign_value * np.sin(angles) * scale


def held(table):
    return table.astype(np.float32).astype(ml_dtypes.bfloat16)


def stacked(real, imaginary):
    return np.block([[real, -imaginary], [imaginary, real]])


def second_tables(size, length, pair):
    real, imaginary = factor(length, size, length, -1.0)
    forward = np.stack(
        [np.concatenate([real, -imaginary], 1), np.concatenate([imaginary, real], 1)], 1
    )
    back_real, back_imaginary = factor(size, length, length, 1.0)
    inverse = np.stack(
        [
            np.concatenate([back_real, back_imaginary], 0),
            np.concatenate([-back_imaginary, back_real], 0),
        ],
        2,
    )
    base = np.arange(length).reshape(-1, 2, pair)
    orders = [base[:, ::step].reshape(-1) for step in (1, -1)]
    return (
        held(np.stack([forward[order].reshape(2 * length, 2 * size) for order in orders])),
        held(np.stack([inverse[:, order].reshape(2 * size, 2 * length) for order in orders])),
    )


def product(a, b):
    return jnp.dot(a, b, preferred_element_type=jnp.float32)


def coil_image_kernel(
    core_ref, image_ref, sensitivity_ref, own_ref, other_ref, image, sensitivity, arrived
):
    core = core_ref[0]
    coils = own_ref.shape[0]
    parts = ((other_ref, (1 - core) * coils), (own_ref, core * coils))
    copies = [pltpu.make_async_copy(image_ref, image, arrived.at[0])]
    copies += [
        pltpu.make_async_copy(
            sensitivity_ref.at[pl.ds(first, coils)], sensitivity.at[i], arrived.at[1 + i]
        )
        for i, (_, first) in enumerate(parts)
    ]
    for copy in copies:
        copy.start()
    copies[0].wait()
    image_real, image_imaginary = image[0, 0], image[1, 0]
    rows = image_real.shape[0]
    for i, (ref, _) in enumerate(parts):
        copies[1 + i].wait()
        for coil in range(coils):
            real = sensitivity[i, coil, 0, 0].astype(jnp.float32)
            imaginary = sensitivity[i, coil, 1, 0].astype(jnp.float32)
            ref[coil, :rows] = (real * image_real - imaginary * image_imaginary).astype(ref.dtype)
            ref[coil, rows:] = (real * image_imaginary + imaginary * image_real).astype(ref.dtype)


def second_kernel(core_ref, table_ref, coils_ref, *refs, own):
    out_ref, built, left = refs[-3:]
    core = core_ref[0]
    coils, groups, rows, width = built.shape
    table = table_ref[core]
    copies = []
    for coil in range(coils):
        built[coil] = (
            product(table, coils_ref[coil]).reshape(groups, rows, width).astype(built.dtype)
        )
        slot = core if own else 1 - core
        copies.append(
            pltpu.make_async_copy(built.at[coil], out_ref.at[:, slot, coil], left.at[coil])
        )
        copies[-1].start()
    for copy in copies:
        copy.wait()
    if not own:

        @pl.when(core == 1)
        def _():
            pl.delay(LAG_NS)


def middle_kernel(
    in_ref, own_ref, other_ref, third_ref, first_ref, back_first_ref, back_third_ref,
    out_ref, lines, both, spread, filtered, back, built, left,
):
    count, coils, rows, width = in_ref.shape
    grid = own_ref.shape[0]
    frequencies = rows // 2
    part_of = [slice(j * count, (j + 1) * count) for j in range(frequencies)]

    def copy_out(coil):
        return pltpu.make_async_copy(built.at[coil], out_ref.at[:, coil], left.at[coil])

    @pl.loop(0, coils)
    def _(coil):
        lines[...] = in_ref[:, coil].astype(jnp.float32).reshape(count * rows, width)
        for j in range(frequencies):
            for part in range(2):
                both[part_of[j], part * width : (part + 1) * width] = lines[
                    pl.ds(2 * j + part, count, stride=rows), :
                ].astype(jnp.bfloat16)
        for j in range(frequencies):
            third = product(both[part_of[j]], third_ref[...]).astype(jnp.bfloat16)
            spread[j, :count] = third[:, :grid]
            spread[j, count:] = third[:, grid:]
        for j in range(frequencies):
            points_ref = (own_ref, other_ref)[j // (frequencies // 2)]
            at = j % (frequencies // 2) * grid
            for part in range(2):
                half = slice(part * grid, (part + 1) * grid)
                spectrum = product(first_ref[half], spread[j])
                filtered[j, half] = (spectrum * points_ref[:, at : at + grid]).astype(jnp.bfloat16)
        for j in range(frequencies):
            first = product(back_first_ref[...], filtered[j]).astype(jnp.bfloat16)
            back[part_of[j], :grid] = first[:count]
            back[part_of[j], grid:] = first[count:]
        for j in range(frequencies):
            result = product(back[part_of[j]], back_third_ref[...])
            for part in range(2):
                lines[pl.ds(2 * j + part, count, stride=rows), :] = result[
                    :, part * width : (part + 1) * width
                ]
        built[coil] = lines[...].reshape(count, rows, width).astype(built.dtype)
        copy_out(coil).start()

    for coil in range(coils):
        copy_out(coil).wait()


def last_kernel(core_ref, in_ref, table_ref, sensitivity_ref, *refs, own):
    out_ref = refs[-1]
    core = core_ref[0]
    groups, _, coils, rows, width = in_ref.shape
    table = table_ref[core]
    slot = core if own else 1 - core
    first = core * coils if own else 0
    size = table.shape[0] // 2
    real_sum = imaginary_sum = 0.0
    for coil in range(coils):
        values = product(table, in_ref[:, slot, coil].reshape(groups * rows, width))
        real = sensitivity_ref[first + coil, 0, 0].astype(jnp.float32)
        imaginary = sensitivity_ref[first + coil, 1, 0].astype(jnp.float32)
        real_sum += real * values[:size] + imaginary * values[size:]
        imaginary_sum += real * values[size:] - imaginary * values[:size]
    if own:
        real_sum += refs[0][0, 0]
        imaginary_sum += refs[0][1, 0]
    out_ref[0, 0] = real_sum
    out_ref[1, 0] = imaginary_sum


def call(kernel, name, out, spaces, operands, scratch=(), flops=0, mib=8, to=VMEM, aliases=None):
    return pl.pallas_call(
        kernel,
        name=name,
        out_shape=out,
        in_specs=[pl.BlockSpec(memory_space=space) for space in spaces],
        out_specs=jax.tree.map(lambda _: pl.BlockSpec(memory_space=to), out),
        scratch_shapes=scratch,
        input_output_aliases=aliases or {},
        compiler_params=pltpu.CompilerParams(vmem_limit_bytes=mib * 2**20),
        cost_estimate=pl.CostEstimate(flops=flops, bytes_accessed=2**20, transcendentals=0),
    )(*operands)


def local(image, sensitivity, kernel, *, groups):
    bf16, f32 = jnp.bfloat16, jnp.float32
    coils, width = sensitivity.shape[0] // 2, image.shape[3]
    size, rows_second = 2 * groups * image.shape[1], image.shape[2]
    grid, pair = kernel.shape[0], kernel.shape[1]
    grid_second, grid_third = 2 * groups * pair, kernel.shape[2]
    rows = 4 * pair
    core = lax.axis_index("core")
    where = core.astype(jnp.int32).reshape(1)
    swap = [(0, 1), (1, 0)]
    shape = jax.ShapeDtypeStruct
    copies = pltpu.SemaphoreType.DMA

    forward_second, inverse_second = second_tables(rows_second, grid_second, pair)
    first_table = held(stacked(*factor(grid, size, grid, -1.0)))
    back_first_table = held(stacked(*factor(size, grid, grid, 1.0)))
    third_table = held(stacked(*factor(grid_third, width, grid_third, -1.0)).T)
    back_third_table = held(stacked(*factor(width, grid_third, grid_third, 1.0)).T)

    partner_points = lax.ppermute(kernel, "core", swap)
    own_coils, other_coils = call(
        coil_image_kernel, "coil_images",
        (shape((coils, 2 * rows_second, width), bf16),) * 2,
        (SMEM, HBM, HBM), (where, image, sensitivity),
        (VMEM(image.shape, f32), VMEM((2, coils, *sensitivity.shape[1:]), bf16), copies((3,))),
        flops=2**20,
    )
    partner_coils = lax.ppermute(other_coils, "core", swap)
    payload = None
    for own, values in ((True, own_coils), (False, partner_coils)):
        if not own:
            values, own_points, partner_points = lax.optimization_barrier(
                (values, kernel, partner_points)
            )
        payload = call(
            functools.partial(second_kernel, own=own), "along_second",
            shape((groups, 2, coils, rows, width), bf16),
            (SMEM, VMEM, VMEM) + (HBM,) * (not own),
            (where, forward_second, values) + (payload,) * (not own),
            (VMEM((coils, groups, rows, width), bf16), copies((coils,))),
            flops=2**28, to=HBM, aliases=None if own else {3: 0},
        )
    own_points = own_points.reshape(grid, pair * grid_third)
    partner_points = partner_points.reshape(grid, pair * grid_third)
    received = lax.all_to_all(payload, "chip", split_axis=0, concat_axis=0, tiled=True)
    returned = call(
        middle_kernel, "middle",
        shape((size, coils, rows, width), bf16),
        (VMEM,) * 7,
        (received.reshape(size, coils, rows, width), own_points, partner_points,
         third_table, first_table, back_first_table, back_third_table),
        (VMEM((size * rows, width), f32), VMEM((2 * pair * size, 2 * width), bf16),
         VMEM((2 * pair, 2 * size, grid_third), bf16), VMEM((2 * pair, 2 * grid, grid_third), bf16),
         VMEM((2 * pair * size, 2 * grid_third), bf16), VMEM((coils, size, rows, width), bf16),
         copies((coils,))),
        flops=2**31, mib=16, to=HBM,
    )
    returned = lax.all_to_all(
        returned.reshape(groups, 2, coils, rows, width), "chip", split_axis=0, concat_axis=0, tiled=True
    )

    ends = 2 * groups - 1
    partner_sensitivity = lax.ppermute(
        lax.dynamic_slice_in_dim(sensitivity, (1 - core) * coils, coils, 0), "core", swap
    )
    beside = lax.ppermute(image, "core", swap) + lax.ppermute(
        image,
        ("chip", "core"),
        [(i, i + 1) for i in range(1, ends, 2)] + [(i, i - 1) for i in range(2, ends + 1, 2)],
    )
    padded = jnp.pad(image, ((0, 0), (0, 0), (1, 1), (1, 1)))
    beside = beside + padded[:, :, 2:, 1:-1] + padded[:, :, :-2, 1:-1]
    beside = beside + padded[:, :, 1:-1, 2:] + padded[:, :, 1:-1, :-2]
    penalty = smooth_weight * (6.0 * image - beside)

    sums = [
        call(
            functools.partial(last_kernel, own=own), "along_second_back",
            shape(image.shape, f32), (SMEM,) + (VMEM,) * len(operands),
            (where, *operands), flops=2**28,
        )
        for own, operands in (
            (False, (returned, inverse_second, partner_sensitivity)),
            (True, (returned, inverse_second, sensitivity, penalty)),
        )
    ]
    return sums[1] + lax.ppermute(sums[0], "core", swap)


def solution(mesh):
    scans, slabs = mesh.devices.shape
    chips = Mesh(mesh.devices.reshape(scans, slabs // 2, 2), (mesh.axis_names[0], "chip", "core"))
    slab = ("chip", "core")
    return jax.shard_map(
        functools.partial(local, groups=slabs // 2),
        mesh=chips,
        in_specs=(
            P(None, slab, mesh.axis_names[0], None),
            P(mesh.axis_names[0], None, slab, None, None),
            P(None, slab, None),
        ),
        out_specs=P(None, slab, mesh.axis_names[0], None),
        check_vma=False,
    )
```

```python
import functools
import math

import jax
import jax.numpy as jnp
import ml_dtypes
import numpy as np
from jax import lax
from jax.experimental import pallas as pl
from jax.experimental.pallas import tpu as pltpu
from jax.sharding import Mesh
from jax.sharding import PartitionSpec as P

smooth_weight = 0.1
LAG_NS = 18000
VMEM, SMEM, HBM = pltpu.VMEM, pltpu.SMEM, pltpu.HBM


def factor(count_out, count_in, length, sign_value):
    phases = np.outer(np.arange(count_out), np.arange(count_in)) % length
    angles = phases * (2.0 * math.pi / length)
    scale = 1.0 / math.sqrt(length)
    return np.cos(angles) * scale, sign_value * np.sin(angles) * scale


def held(table):
    return table.astype(np.float32).astype(ml_dtypes.bfloat16)


def stacked(real, imaginary):
    return np.block([[real, -imaginary], [imaginary, real]])


def second_tables(size, length):
    real, imaginary = factor(length, size, length, -1.0)
    forward = np.stack(
        [np.concatenate([real, -imaginary], 1), np.concatenate([imaginary, real], 1)], 1
    )
    real, imaginary = factor(size, length, length, 1.0)
    inverse = np.stack(
        [np.concatenate([real, imaginary], 0), np.concatenate([-imaginary, real], 0)], 2
    )
    return held(forward.reshape(2 * length, -1)), held(inverse.reshape(-1, 2 * length))


def product(a, b):
    return jnp.dot(a, b, preferred_element_type=jnp.float32)


def coil_image_kernel(core_ref, image_ref, sensitivity_ref, own_ref, other_ref):
    core = core_ref[0]
    coils = own_ref.shape[0]
    image_real, image_imaginary = image_ref[0, 0], image_ref[1, 0]
    rows = image_real.shape[0]
    for ref, first in ((other_ref, (1 - core) * coils), (own_ref, core * coils)):
        for coil in range(coils):
            real = sensitivity_ref[first + coil, 0, 0].astype(jnp.float32)
            imaginary = sensitivity_ref[first + coil, 1, 0].astype(jnp.float32)
            ref[coil, :rows] = (real * image_real - imaginary * image_imaginary).astype(ref.dtype)
            ref[coil, rows:] = (real * image_imaginary + imaginary * image_real).astype(ref.dtype)


def own_second_kernel(table_ref, coils_ref, built_ref):
    table = table_ref[...]
    coils, groups, rows, width = built_ref.shape
    for coil in range(coils):
        built_ref[coil] = (
            product(table, coils_ref[coil]).reshape(groups, rows, width).astype(built_ref.dtype)
        )


def second_kernel(core_ref, table_ref, coils_ref, own_ref, out_ref, built, left):
    core = core_ref[0]
    coils, groups, rows, width = built.shape
    table = table_ref[...]

    def copy_out(values, slot, coil, which):
        return pltpu.make_async_copy(values, out_ref.at[:, slot, coil], left.at[which, coil])

    for coil in range(coils):
        copy_out(own_ref.at[coil], core, coil, 0).start()
    for coil in range(coils):
        built[coil] = (
            product(table, coils_ref[coil]).reshape(groups, rows, width).astype(built.dtype)
        )
        copy_out(built.at[coil], 1 - core, coil, 1).start()
    for coil in range(coils):
        copy_out(own_ref.at[coil], core, coil, 0).wait()
        copy_out(built.at[coil], 1 - core, coil, 1).wait()

    @pl.when(core == 1)
    def _():
        pl.delay(LAG_NS)


def middle_kernel(
    core_ref, in_ref, points_ref, third_ref, first_ref, back_first_ref, back_third_ref,
    out_ref, lines, both, spread, filtered, back, built, left,
):
    count, coils, rows, width = in_ref.shape
    grid = points_ref.shape[1]
    core = core_ref[0]
    frequencies = rows // 2
    part_of = [slice(j * count, (j + 1) * count) for j in range(frequencies)]

    def copy_out(coil):
        return pltpu.make_async_copy(built.at[coil], out_ref.at[:, coil], left.at[coil])

    @pl.loop(0, coils)
    def _(coil):
        lines[...] = in_ref[:, coil].astype(jnp.float32).reshape(count * rows, width)
        for j in range(frequencies):
            for part in range(2):
                both[part_of[j], part * width : (part + 1) * width] = lines[
                    pl.ds(2 * j + part, count, stride=rows), :
                ].astype(jnp.bfloat16)
        for j in range(frequencies):
            third = product(both[part_of[j]], third_ref[...]).astype(jnp.bfloat16)
            spread[j, :count] = third[:, :grid]
            spread[j, count:] = third[:, grid:]
        for j in range(frequencies):
            place = core if j < frequencies // 2 else 1 - core
            at = j % (frequencies // 2) * grid
            for part in range(2):
                half = slice(part * grid, (part + 1) * grid)
                spectrum = product(first_ref[half], spread[j])
                filtered[j, half] = (
                    spectrum * points_ref[place, :, at : at + grid]
                ).astype(jnp.bfloat16)
        for j in range(frequencies):
            first = product(back_first_ref[...], filtered[j]).astype(jnp.bfloat16)
            back[part_of[j], :grid] = first[:count]
            back[part_of[j], grid:] = first[count:]
        for j in range(frequencies):
            result = product(back[part_of[j]], back_third_ref[...])
            for part in range(2):
                lines[pl.ds(2 * j + part, count, stride=rows), :] = result[
                    :, part * width : (part + 1) * width
                ]
        built[coil] = lines[...].reshape(count, rows, width).astype(built.dtype)
        copy_out(coil).start()

    for coil in range(coils):
        copy_out(coil).wait()


def last_kernel(core_ref, in_ref, table_ref, sensitivity_ref, *refs, own):
    out_ref = refs[-1]
    core = core_ref[0]
    groups, _, coils, rows, width = in_ref.shape
    table = table_ref[...]
    slot = core if own else 1 - core
    first = core * coils if own else 0
    size = table.shape[0] // 2
    real_sum = imaginary_sum = 0.0
    for coil in range(coils):
        values = product(table, in_ref[:, slot, coil].reshape(groups * rows, width))
        real = sensitivity_ref[first + coil, 0, 0].astype(jnp.float32)
        imaginary = sensitivity_ref[first + coil, 1, 0].astype(jnp.float32)
        real_sum += real * values[:size] + imaginary * values[size:]
        imaginary_sum += real * values[size:] - imaginary * values[:size]
    if own:
        real_sum += refs[0][0, 0]
        imaginary_sum += refs[0][1, 0]
    out_ref[0, 0] = real_sum
    out_ref[1, 0] = imaginary_sum


def call(kernel, name, out, spaces, operands, scratch=(), flops=0, mib=8, to=VMEM):
    return pl.pallas_call(
        kernel,
        name=name,
        out_shape=out,
        in_specs=[pl.BlockSpec(memory_space=space) for space in spaces],
        out_specs=jax.tree.map(lambda _: pl.BlockSpec(memory_space=to), out),
        scratch_shapes=scratch,
        compiler_params=pltpu.CompilerParams(vmem_limit_bytes=mib * 2**20),
        cost_estimate=pl.CostEstimate(flops=flops, bytes_accessed=2**20, transcendentals=0),
    )(*operands)


def local(image, sensitivity, kernel, *, groups):
    bf16, f32 = jnp.bfloat16, jnp.float32
    coils, width = sensitivity.shape[0] // 2, image.shape[3]
    size, rows_second = 2 * groups * image.shape[1], image.shape[2]
    grid, pair = kernel.shape[0], kernel.shape[1]
    grid_second, grid_third = 2 * groups * pair, kernel.shape[2]
    rows = 4 * pair
    core = lax.axis_index("core")
    where = core.astype(jnp.int32).reshape(1)
    swap = [(0, 1), (1, 0)]
    shape = jax.ShapeDtypeStruct
    copies = pltpu.SemaphoreType.DMA

    forward_second, inverse_second = second_tables(rows_second, grid_second)
    first_table = held(stacked(*factor(grid, size, grid, -1.0)))
    back_first_table = held(stacked(*factor(size, grid, grid, 1.0)))
    third_table = held(stacked(*factor(grid_third, width, grid_third, -1.0)).T)
    back_third_table = held(stacked(*factor(width, grid_third, grid_third, 1.0)).T)

    partner_points = lax.ppermute(kernel, "core", swap)
    own_coils, other_coils = call(
        coil_image_kernel, "coil_images",
        (shape((coils, 2 * rows_second, width), bf16),) * 2,
        (SMEM, VMEM, VMEM), (where, image, sensitivity),
        flops=2**20,
    )
    partner_coils = lax.ppermute(other_coils, "core", swap)
    own_built = call(
        own_second_kernel, "along_second",
        shape((coils, groups, rows, width), bf16),
        (VMEM, VMEM), (forward_second, own_coils), flops=2**28,
    )
    partner_coils, own_built, own_points, partner_points = lax.optimization_barrier(
        (partner_coils, own_built, kernel, partner_points)
    )
    payload = call(
        second_kernel, "along_second",
        shape((groups, 2, coils, rows, width), bf16),
        (SMEM, VMEM, VMEM, VMEM), (where, forward_second, partner_coils, own_built),
        (VMEM((coils, groups, rows, width), bf16), copies((2, coils))),
        flops=2**28, to=HBM,
    )
    points = jnp.stack([own_points, partner_points]).reshape(2, grid, pair * grid_third)
    received = lax.all_to_all(payload, "chip", split_axis=0, concat_axis=0, tiled=True)
    returned = call(
        middle_kernel, "middle",
        shape((size, coils, rows, width), bf16),
        (SMEM,) + (VMEM,) * 6,
        (where, received.reshape(size, coils, rows, width), points,
         third_table, first_table, back_first_table, back_third_table),
        (VMEM((size * rows, width), f32), VMEM((2 * pair * size, 2 * width), bf16),
         VMEM((2 * pair, 2 * size, grid_third), bf16), VMEM((2 * pair, 2 * grid, grid_third), bf16),
         VMEM((2 * pair * size, 2 * grid_third), bf16), VMEM((coils, size, rows, width), bf16),
         copies((coils,))),
        flops=2**31, mib=16, to=HBM,
    )
    returned = lax.all_to_all(
        returned.reshape(groups, 2, coils, rows, width), "chip", split_axis=0, concat_axis=0, tiled=True
    )

    ends = 2 * groups - 1
    outer = lax.ppermute(
        image.astype(bf16),
        ("chip", "core"),
        [(i, i + 1) for i in range(1, ends, 2)] + [(i, i - 1) for i in range(2, ends + 1, 2)],
    )
    partner_sensitivity = lax.ppermute(
        lax.dynamic_slice_in_dim(sensitivity, (1 - core) * coils, coils, 0), "core", swap
    )
    beside = lax.ppermute(image, "core", swap) + outer.astype(f32)
    padded = jnp.pad(image, ((0, 0), (0, 0), (1, 1), (1, 1)))
    beside = beside + padded[:, :, 2:, 1:-1] + padded[:, :, :-2, 1:-1]
    beside = beside + padded[:, :, 1:-1, 2:] + padded[:, :, 1:-1, :-2]
    penalty = smooth_weight * (6.0 * image - beside)

    sums = [
        call(
            functools.partial(last_kernel, own=own), "along_second_back",
            shape(image.shape, f32), (SMEM,) + (VMEM,) * len(operands),
            (where, *operands), flops=2**28,
        )
        for own, operands in (
            (False, (returned, inverse_second, partner_sensitivity)),
            (True, (returned, inverse_second, sensitivity, penalty)),
        )
    ]
    return sums[1] + lax.ppermute(sums[0], "core", swap)


def solution(mesh):
    scans, slabs = mesh.devices.shape
    chips = Mesh(mesh.devices.reshape(scans, slabs // 2, 2), (mesh.axis_names[0], "chip", "core"))
    slab = ("chip", "core")
    return jax.shard_map(
        functools.partial(local, groups=slabs // 2),
        mesh=chips,
        in_specs=(
            P(None, slab, mesh.axis_names[0], None),
            P(mesh.axis_names[0], None, slab, None, None),
            P(None, slab, None),
        ),
        out_specs=P(None, slab, mesh.axis_names[0], None),
        check_vma=False,
    )
```

```python
import functools
import math

import jax
import jax.numpy as jnp
import ml_dtypes
import numpy as np
from jax import lax
from jax.experimental import pallas as pl
from jax.experimental.pallas import tpu as pltpu
from jax.sharding import Mesh
from jax.sharding import PartitionSpec as P

smooth_weight = 0.1
LAG_NS = 18000
VMEM, SMEM, HBM = pltpu.VMEM, pltpu.SMEM, pltpu.HBM


def factor(count_out, count_in, length, sign_value):
    phases = np.outer(np.arange(count_out), np.arange(count_in)) % length
    angles = phases * (2.0 * math.pi / length)
    scale = 1.0 / math.sqrt(length)
    return np.cos(angles) * scale, sign_value * np.sin(angles) * scale


def held(table):
    return table.astype(np.float32).astype(ml_dtypes.bfloat16)


def stacked(real, imaginary):
    return np.block([[real, -imaginary], [imaginary, real]])


def second_tables(size, length):
    real, imaginary = factor(length, size, length, -1.0)
    forward = np.stack(
        [np.concatenate([real, -imaginary], 1), np.concatenate([imaginary, real], 1)], 1
    )
    real, imaginary = factor(size, length, length, 1.0)
    inverse = np.stack(
        [np.concatenate([real, imaginary], 0), np.concatenate([-imaginary, real], 0)], 2
    )
    return held(forward.reshape(2 * length, -1)), held(inverse.reshape(-1, 2 * length))


def product(a, b):
    return jnp.dot(a, b, preferred_element_type=jnp.float32)


def opening_kernel(out_ref):
    out_ref[...] = jnp.zeros_like(out_ref)


def coil_image_kernel(core_ref, _, image_ref, sensitivity_ref, own_ref, other_ref):
    core = core_ref[0]
    coils = own_ref.shape[0]
    image_real, image_imaginary = image_ref[0, 0], image_ref[1, 0]
    rows = image_real.shape[0]
    for ref, first in ((other_ref, (1 - core) * coils), (own_ref, core * coils)):
        for coil in range(coils):
            real = sensitivity_ref[first + coil, 0, 0].astype(jnp.float32)
            imaginary = sensitivity_ref[first + coil, 1, 0].astype(jnp.float32)
            ref[coil, :rows] = (real * image_real - imaginary * image_imaginary).astype(ref.dtype)
            ref[coil, rows:] = (real * image_imaginary + imaginary * image_real).astype(ref.dtype)


def own_second_kernel(table_ref, coils_ref, built_ref):
    table = table_ref[...]
    coils, groups, rows, width = built_ref.shape
    for coil in range(coils):
        built_ref[coil] = (
            product(table, coils_ref[coil]).reshape(groups, rows, width).astype(built_ref.dtype)
        )


def second_kernel(core_ref, table_ref, coils_ref, own_ref, out_ref, built, left):
    core = core_ref[0]
    coils, groups, rows, width = built.shape
    table = table_ref[...]

    def copy_out(values, slot, coil, which):
        return pltpu.make_async_copy(values, out_ref.at[:, slot, coil], left.at[which, coil])

    for coil in range(coils):
        copy_out(own_ref.at[coil], core, coil, 0).start()
    for coil in range(coils):
        built[coil] = (
            product(table, coils_ref[coil]).reshape(groups, rows, width).astype(built.dtype)
        )
        copy_out(built.at[coil], 1 - core, coil, 1).start()
    for coil in range(coils):
        copy_out(own_ref.at[coil], core, coil, 0).wait()
        copy_out(built.at[coil], 1 - core, coil, 1).wait()

    @pl.when(core == 1)
    def _():
        pl.delay(LAG_NS)


def middle_kernel(
    core_ref, in_ref, points_ref, third_ref, first_ref, back_first_ref, back_third_ref,
    out_ref, lines, both, spread, filtered, back, built, left,
):
    count, coils, rows, width = in_ref.shape
    grid = points_ref.shape[1]
    core = core_ref[0]
    frequencies = rows // 2
    part_of = [slice(j * count, (j + 1) * count) for j in range(frequencies)]

    def copy_out(coil):
        return pltpu.make_async_copy(built.at[coil], out_ref.at[:, coil], left.at[coil])

    @pl.loop(0, coils)
    def _(coil):
        lines[...] = in_ref[:, coil].astype(jnp.float32).reshape(count * rows, width)
        for j in range(frequencies):
            for part in range(2):
                both[part_of[j], part * width : (part + 1) * width] = lines[
                    pl.ds(2 * j + part, count, stride=rows), :
                ].astype(jnp.bfloat16)
        for j in range(frequencies):
            third = product(both[part_of[j]], third_ref[...]).astype(jnp.bfloat16)
            spread[j, :count] = third[:, :grid]
            spread[j, count:] = third[:, grid:]
        for j in range(frequencies):
            place = core if j < frequencies // 2 else 1 - core
            at = j % (frequencies // 2) * grid
            for part in range(2):
                half = slice(part * grid, (part + 1) * grid)
                spectrum = product(first_ref[half], spread[j])
                filtered[j, half] = (
                    spectrum * points_ref[place, :, at : at + grid]
                ).astype(jnp.bfloat16)
        for j in range(frequencies):
            first = product(back_first_ref[...], filtered[j]).astype(jnp.bfloat16)
            back[part_of[j], :grid] = first[:count]
            back[part_of[j], grid:] = first[count:]
        for j in range(frequencies):
            result = product(back[part_of[j]], back_third_ref[...])
            for part in range(2):
                lines[pl.ds(2 * j + part, count, stride=rows), :] = result[
                    :, part * width : (part + 1) * width
                ]
        built[coil] = lines[...].reshape(count, rows, width).astype(built.dtype)
        copy_out(coil).start()

    for coil in range(coils):
        copy_out(coil).wait()


def last_kernel(core_ref, in_ref, table_ref, sensitivity_ref, *refs, own):
    out_ref = refs[-1]
    core = core_ref[0]
    groups, _, coils, rows, width = in_ref.shape
    table = table_ref[...]
    slot = core if own else 1 - core
    first = core * coils if own else 0
    size = table.shape[0] // 2
    real_sum = imaginary_sum = 0.0
    for coil in range(coils):
        values = product(table, in_ref[:, slot, coil].reshape(groups * rows, width))
        real = sensitivity_ref[first + coil, 0, 0].astype(jnp.float32)
        imaginary = sensitivity_ref[first + coil, 1, 0].astype(jnp.float32)
        real_sum += real * values[:size] + imaginary * values[size:]
        imaginary_sum += real * values[size:] - imaginary * values[:size]
    if own:
        real_sum += refs[0][0, 0]
        imaginary_sum += refs[0][1, 0]
    out_ref[0, 0] = real_sum
    out_ref[1, 0] = imaginary_sum


def call(kernel, name, out, spaces, operands, scratch=(), flops=0, mib=8, to=VMEM):
    return pl.pallas_call(
        kernel,
        name=name,
        out_shape=out,
        in_specs=[pl.BlockSpec(memory_space=space) for space in spaces],
        out_specs=jax.tree.map(lambda _: pl.BlockSpec(memory_space=to), out),
        scratch_shapes=scratch,
        compiler_params=pltpu.CompilerParams(vmem_limit_bytes=mib * 2**20),
        cost_estimate=pl.CostEstimate(flops=flops, bytes_accessed=2**20, transcendentals=0),
    )(*operands)


def local(image, sensitivity, kernel, *, groups):
    bf16, f32 = jnp.bfloat16, jnp.float32
    coils, width = sensitivity.shape[0] // 2, image.shape[3]
    size, rows_second = 2 * groups * image.shape[1], image.shape[2]
    grid, pair = kernel.shape[0], kernel.shape[1]
    grid_second, grid_third = 2 * groups * pair, kernel.shape[2]
    rows = 4 * pair
    core = lax.axis_index("core")
    where = core.astype(jnp.int32).reshape(1)
    swap = [(0, 1), (1, 0)]
    shape = jax.ShapeDtypeStruct
    copies = pltpu.SemaphoreType.DMA

    forward_second, inverse_second = second_tables(rows_second, grid_second)
    first_table = held(stacked(*factor(grid, size, grid, -1.0)))
    back_first_table = held(stacked(*factor(size, grid, grid, 1.0)))
    third_table = held(stacked(*factor(grid_third, width, grid_third, -1.0)).T)
    back_third_table = held(stacked(*factor(width, grid_third, grid_third, 1.0)).T)

    partner_points = lax.ppermute(kernel, "core", swap)
    opened = call(opening_kernel, "opening", shape((8, 128), f32), (), (), flops=2**30)
    own_coils, other_coils = call(
        coil_image_kernel, "coil_images",
        (shape((coils, 2 * rows_second, width), bf16),) * 2,
        (SMEM, VMEM, VMEM, VMEM), (where, opened, image, sensitivity),
        flops=2**20,
    )
    partner_coils = lax.ppermute(other_coils, "core", swap)
    own_built = call(
        own_second_kernel, "along_second",
        shape((coils, groups, rows, width), bf16),
        (VMEM, VMEM), (forward_second, own_coils), flops=2**28,
    )
    partner_coils, own_built, own_points, partner_points = lax.optimization_barrier(
        (partner_coils, own_built, kernel, partner_points)
    )
    payload = call(
        second_kernel, "along_second",
        shape((groups, 2, coils, rows, width), bf16),
        (SMEM, VMEM, VMEM, VMEM), (where, forward_second, partner_coils, own_built),
        (VMEM((coils, groups, rows, width), bf16), copies((2, coils))),
        flops=2**28, to=HBM,
    )
    points = jnp.stack([own_points, partner_points]).reshape(2, grid, pair * grid_third)
    received = lax.all_to_all(payload, "chip", split_axis=0, concat_axis=0, tiled=True)
    returned = call(
        middle_kernel, "middle",
        shape((size, coils, rows, width), bf16),
        (SMEM,) + (VMEM,) * 6,
        (where, received.reshape(size, coils, rows, width), points,
         third_table, first_table, back_first_table, back_third_table),
        (VMEM((size * rows, width), f32), VMEM((2 * pair * size, 2 * width), bf16),
         VMEM((2 * pair, 2 * size, grid_third), bf16), VMEM((2 * pair, 2 * grid, grid_third), bf16),
         VMEM((2 * pair * size, 2 * grid_third), bf16), VMEM((coils, size, rows, width), bf16),
         copies((coils,))),
        flops=2**31, mib=16, to=HBM,
    )
    returned = lax.all_to_all(
        returned.reshape(groups, 2, coils, rows, width), "chip", split_axis=0, concat_axis=0, tiled=True
    )

    ends = 2 * groups - 1
    outer = lax.ppermute(
        image.astype(bf16),
        ("chip", "core"),
        [(i, i + 1) for i in range(1, ends, 2)] + [(i, i - 1) for i in range(2, ends + 1, 2)],
    )
    partner_sensitivity = lax.ppermute(
        lax.dynamic_slice_in_dim(sensitivity, (1 - core) * coils, coils, 0), "core", swap
    )
    beside = lax.ppermute(image, "core", swap) + outer.astype(f32)
    padded = jnp.pad(image, ((0, 0), (0, 0), (1, 1), (1, 1)))
    beside = beside + padded[:, :, 2:, 1:-1] + padded[:, :, :-2, 1:-1]
    beside = beside + padded[:, :, 1:-1, 2:] + padded[:, :, 1:-1, :-2]
    penalty = smooth_weight * (6.0 * image - beside)

    sums = [
        call(
            functools.partial(last_kernel, own=own), "along_second_back",
            shape(image.shape, f32), (SMEM,) + (VMEM,) * len(operands),
            (where, *operands), flops=2**28,
        )
        for own, operands in (
            (False, (returned, inverse_second, partner_sensitivity)),
            (True, (returned, inverse_second, sensitivity, penalty)),
        )
    ]
    return sums[1] + lax.ppermute(sums[0], "core", swap)


def solution(mesh):
    scans, slabs = mesh.devices.shape
    chips = Mesh(mesh.devices.reshape(scans, slabs // 2, 2), (mesh.axis_names[0], "chip", "core"))
    slab = ("chip", "core")
    return jax.shard_map(
        functools.partial(local, groups=slabs // 2),
        mesh=chips,
        in_specs=(
            P(None, slab, mesh.axis_names[0], None),
            P(mesh.axis_names[0], None, slab, None, None),
            P(None, slab, None),
        ),
        out_specs=P(None, slab, mesh.axis_names[0], None),
        check_vma=False,
    )
```

```python
import functools
import math

import jax
import jax.numpy as jnp
import ml_dtypes
import numpy as np
from jax import lax
from jax.experimental import pallas as pl
from jax.experimental.pallas import tpu as pltpu
from jax.sharding import Mesh
from jax.sharding import PartitionSpec as P

smooth_weight = 0.1
LAG_NS = 18000
VMEM, SMEM, HBM = pltpu.VMEM, pltpu.SMEM, pltpu.HBM


def factor(count_out, count_in, length, sign_value):
    phases = np.outer(np.arange(count_out), np.arange(count_in)) % length
    angles = phases * (2.0 * math.pi / length)
    scale = 1.0 / math.sqrt(length)
    return np.cos(angles) * scale, sign_value * np.sin(angles) * scale


def held(table):
    return table.astype(np.float32).astype(ml_dtypes.bfloat16)


def stacked(real, imaginary):
    return np.block([[real, -imaginary], [imaginary, real]])


def second_tables(size, length):
    real, imaginary = factor(length, size, length, -1.0)
    forward = np.stack(
        [np.concatenate([real, -imaginary], 1), np.concatenate([imaginary, real], 1)], 1
    )
    real, imaginary = factor(size, length, length, 1.0)
    inverse = np.stack(
        [np.concatenate([real, imaginary], 0), np.concatenate([-imaginary, real], 0)], 2
    )
    return held(forward.reshape(2 * length, -1)), held(inverse.reshape(-1, 2 * length))


def product(a, b):
    return jnp.dot(a, b, preferred_element_type=jnp.float32)


def opening_kernel(out_ref):
    out_ref[...] = jnp.zeros_like(out_ref)


def coil_image_kernel(core_ref, _, image_ref, sensitivity_ref, own_ref, other_ref):
    core = core_ref[0]
    coils = own_ref.shape[0]
    image_real, image_imaginary = image_ref[0, 0], image_ref[1, 0]
    rows = image_real.shape[0]
    for ref, first in ((other_ref, (1 - core) * coils), (own_ref, core * coils)):
        for coil in range(coils):
            real = sensitivity_ref[first + coil, 0, 0].astype(jnp.float32)
            imaginary = sensitivity_ref[first + coil, 1, 0].astype(jnp.float32)
            ref[coil, :rows] = (real * image_real - imaginary * image_imaginary).astype(ref.dtype)
            ref[coil, rows:] = (real * image_imaginary + imaginary * image_real).astype(ref.dtype)


def own_second_kernel(table_ref, coils_ref, built_ref):
    table = table_ref[...]
    coils, groups, rows, width = built_ref.shape
    for coil in range(coils):
        built_ref[coil] = (
            product(table, coils_ref[coil]).reshape(groups, rows, width).astype(built_ref.dtype)
        )


def second_kernel(core_ref, table_ref, coils_ref, own_ref, out_ref, built, left):
    core = core_ref[0]
    coils, groups, rows, width = built.shape
    table = table_ref[...]

    def copy_out(values, slot, coil, which):
        return pltpu.make_async_copy(values, out_ref.at[:, slot, coil], left.at[which, coil])

    for coil in range(coils):
        copy_out(own_ref.at[coil], core, coil, 0).start()
    for coil in range(coils):
        built[coil] = (
            product(table, coils_ref[coil]).reshape(groups, rows, width).astype(built.dtype)
        )
        copy_out(built.at[coil], 1 - core, coil, 1).start()
    for coil in range(coils):
        copy_out(own_ref.at[coil], core, coil, 0).wait()
        copy_out(built.at[coil], 1 - core, coil, 1).wait()

    @pl.when(core == 1)
    def _():
        pl.delay(LAG_NS)


def middle_kernel(
    in_ref, points_ref, third_ref, first_ref, back_first_ref, back_third_ref,
    out_ref, lines, both, spread, filtered, back, built, left,
):
    count, coils, rows, width = in_ref.shape
    grid = points_ref.shape[1]
    frequencies = rows // 2
    part_of = [slice(j * count, (j + 1) * count) for j in range(frequencies)]

    def copy_out(coil):
        return pltpu.make_async_copy(built.at[coil], out_ref.at[:, coil], left.at[coil])

    @pl.loop(0, coils)
    def _(coil):
        lines[...] = in_ref[:, coil].astype(jnp.float32).reshape(count * rows, width)
        for j in range(frequencies):
            for part in range(2):
                both[part_of[j], part * width : (part + 1) * width] = lines[
                    pl.ds(2 * j + part, count, stride=rows), :
                ].astype(jnp.bfloat16)
        for j in range(frequencies):
            third = product(both[part_of[j]], third_ref[...]).astype(jnp.bfloat16)
            spread[j, :count] = third[:, :grid]
            spread[j, count:] = third[:, grid:]
        for j in range(frequencies):
            place = j // (frequencies // 2)
            at = j % (frequencies // 2) * grid
            for part in range(2):
                half = slice(part * grid, (part + 1) * grid)
                spectrum = product(first_ref[half], spread[j])
                filtered[j, half] = (
                    spectrum * points_ref[place, :, at : at + grid]
                ).astype(jnp.bfloat16)
        for j in range(frequencies):
            first = product(back_first_ref[...], filtered[j]).astype(jnp.bfloat16)
            back[part_of[j], :grid] = first[:count]
            back[part_of[j], grid:] = first[count:]
        for j in range(frequencies):
            result = product(back[part_of[j]], back_third_ref[...])
            for part in range(2):
                lines[pl.ds(2 * j + part, count, stride=rows), :] = result[
                    :, part * width : (part + 1) * width
                ]
        built[coil] = lines[...].reshape(count, rows, width).astype(built.dtype)
        copy_out(coil).start()

    for coil in range(coils):
        copy_out(coil).wait()


def last_kernel(core_ref, in_ref, table_ref, sensitivity_ref, *refs, own):
    out_ref = refs[-1]
    core = core_ref[0]
    groups, _, coils, rows, width = in_ref.shape
    table = table_ref[...]
    slot = core if own else 1 - core
    first = core * coils if own else 0
    size = table.shape[0] // 2
    real_sum = imaginary_sum = 0.0
    for coil in range(coils):
        values = product(table, in_ref[:, slot, coil].reshape(groups * rows, width))
        real = sensitivity_ref[first + coil, 0, 0].astype(jnp.float32)
        imaginary = sensitivity_ref[first + coil, 1, 0].astype(jnp.float32)
        real_sum += real * values[:size] + imaginary * values[size:]
        imaginary_sum += real * values[size:] - imaginary * values[:size]
    if own:
        real_sum += refs[0][0, 0]
        imaginary_sum += refs[0][1, 0]
    out_ref[0, 0] = real_sum
    out_ref[1, 0] = imaginary_sum


def call(kernel, name, out, spaces, operands, scratch=(), flops=0, mib=8, to=VMEM):
    return pl.pallas_call(
        kernel,
        name=name,
        out_shape=out,
        in_specs=[pl.BlockSpec(memory_space=space) for space in spaces],
        out_specs=jax.tree.map(lambda _: pl.BlockSpec(memory_space=to), out),
        scratch_shapes=scratch,
        compiler_params=pltpu.CompilerParams(vmem_limit_bytes=mib * 2**20),
        cost_estimate=pl.CostEstimate(flops=flops, bytes_accessed=2**20, transcendentals=0),
    )(*operands)


def local(image, sensitivity, kernel, *, groups):
    bf16, f32 = jnp.bfloat16, jnp.float32
    coils, width = sensitivity.shape[0] // 2, image.shape[3]
    size, rows_second = 2 * groups * image.shape[1], image.shape[2]
    grid, pair = kernel.shape[0], kernel.shape[1]
    grid_second, grid_third = 2 * groups * pair, kernel.shape[2]
    rows = 4 * pair
    core = lax.axis_index("core")
    where = core.astype(jnp.int32).reshape(1)
    swap = [(0, 1), (1, 0)]
    shape = jax.ShapeDtypeStruct
    copies = pltpu.SemaphoreType.DMA

    forward_second, inverse_second = second_tables(rows_second, grid_second)
    first_table = held(stacked(*factor(grid, size, grid, -1.0)))
    back_first_table = held(stacked(*factor(size, grid, grid, 1.0)))
    third_table = held(stacked(*factor(grid_third, width, grid_third, -1.0)).T)
    back_third_table = held(stacked(*factor(width, grid_third, grid_third, 1.0)).T)

    partner_points = lax.ppermute(kernel, "core", swap)
    opened = call(opening_kernel, "opening", shape((8, 128), f32), (), (), flops=2**30)
    own_coils, other_coils = call(
        coil_image_kernel, "coil_images",
        (shape((coils, 2 * rows_second, width), bf16),) * 2,
        (SMEM, VMEM, VMEM, VMEM), (where, opened, image, sensitivity),
        flops=2**20,
    )
    partner_coils = lax.ppermute(other_coils, "core", swap)
    own_built = call(
        own_second_kernel, "along_second",
        shape((coils, groups, rows, width), bf16),
        (VMEM, VMEM), (forward_second, own_coils), flops=2**28,
    )
    partner_coils, own_built, own_points, partner_points = lax.optimization_barrier(
        (partner_coils, own_built, kernel, partner_points)
    )
    payload = call(
        second_kernel, "along_second",
        shape((groups, 2, coils, rows, width), bf16),
        (SMEM, VMEM, VMEM, VMEM), (where, forward_second, partner_coils, own_built),
        (VMEM((coils, groups, rows, width), bf16), copies((2, coils))),
        flops=2**28, to=HBM,
    )
    first_points = jnp.where(core == 0, own_points, partner_points)
    second_points = jnp.where(core == 0, partner_points, own_points)
    points = jnp.stack([first_points, second_points]).reshape(2, grid, pair * grid_third)
    received = lax.all_to_all(payload, "chip", split_axis=0, concat_axis=0, tiled=True)
    returned = call(
        middle_kernel, "middle",
        shape((size, coils, rows, width), bf16),
        (VMEM,) * 6,
        (received.reshape(size, coils, rows, width), points,
         third_table, first_table, back_first_table, back_third_table),
        (VMEM((size * rows, width), f32), VMEM((2 * pair * size, 2 * width), bf16),
         VMEM((2 * pair, 2 * size, grid_third), bf16), VMEM((2 * pair, 2 * grid, grid_third), bf16),
         VMEM((2 * pair * size, 2 * grid_third), bf16), VMEM((coils, size, rows, width), bf16),
         copies((coils,))),
        flops=2**31, mib=16, to=HBM,
    )
    returned = lax.all_to_all(
        returned.reshape(groups, 2, coils, rows, width), "chip", split_axis=0, concat_axis=0, tiled=True
    )

    ends = 2 * groups - 1
    outer = lax.ppermute(
        image.astype(bf16),
        ("chip", "core"),
        [(i, i + 1) for i in range(1, ends, 2)] + [(i, i - 1) for i in range(2, ends + 1, 2)],
    )
    partner_sensitivity = lax.ppermute(
        lax.dynamic_slice_in_dim(sensitivity, (1 - core) * coils, coils, 0), "core", swap
    )
    beside = lax.ppermute(image, "core", swap) + outer.astype(f32)
    padded = jnp.pad(image, ((0, 0), (0, 0), (1, 1), (1, 1)))
    beside = beside + padded[:, :, 2:, 1:-1] + padded[:, :, :-2, 1:-1]
    beside = beside + padded[:, :, 1:-1, 2:] + padded[:, :, 1:-1, :-2]
    penalty = smooth_weight * (6.0 * image - beside)

    sums = [
        call(
            functools.partial(last_kernel, own=own), "along_second_back",
            shape(image.shape, f32), (SMEM,) + (VMEM,) * len(operands),
            (where, *operands), flops=2**28,
        )
        for own, operands in (
            (False, (returned, inverse_second, partner_sensitivity)),
            (True, (returned, inverse_second, sensitivity, penalty)),
        )
    ]
    return sums[1] + lax.ppermute(sums[0], "core", swap)


def solution(mesh):
    scans, slabs = mesh.devices.shape
    chips = Mesh(mesh.devices.reshape(scans, slabs // 2, 2), (mesh.axis_names[0], "chip", "core"))
    slab = ("chip", "core")
    return jax.shard_map(
        functools.partial(local, groups=slabs // 2),
        mesh=chips,
        in_specs=(
            P(None, slab, mesh.axis_names[0], None),
            P(mesh.axis_names[0], None, slab, None, None),
            P(None, slab, None),
        ),
        out_specs=P(None, slab, mesh.axis_names[0], None),
        check_vma=False,
    )
```
